32 devices in a mesh: group: 2 (over y), dp: 4 (over z), tensor: 4 (over x, core).
Axes of the slice: x: 2, y: 2, z: 4, core: 2. Of those that a mesh axis runs over, the one named last changes fastest.
Arguments:
- queries: bfloat16 [32, 4, 8192], P(('group', 'dp')), may hold values from -330 to 330
- keys: bfloat16 [32, 8, 512, 128], P(('group', 'dp'), None, 'tensor'), may hold values from -12 to 12
- values: bfloat16 [32, 8, 512, 128], P(('group', 'dp'), None, 'tensor'), may hold values from -12 to 12
- cached_length: int32 [32], P(('group', 'dp')), may hold values from 2 to 508
- out_weight: bfloat16 [8192, 8192], P('tensor', ('group', 'dp')), may hold values from -0.0625 to 0.0625
Outputs:
- projected: bfloat16 [128, 2, 4096], P(('group', 'tensor'), None, 'dp')
The draws below stay inside these ranges and needn't reach their ends.
Inputs may be any that keep to these rules, and one draw needn't show every extreme that they name: The keys and values of row r's 4 new tokens sit at positions cached_length[r] to cached_length[r] + 3.
All inputs are finite; a program needn't handle non-finite values.
Results may differ from the reference program's by a relative error of at most 0.018.
Values may be sent and summed in bfloat16 or wider, within the bound.
No kernel may reach another device: no remote copies, remote signals or barrier semaphores. Data moves between devices by JAX's collectives and lax.ppermute only.
A program may use at most 64 MiB of HBM per device.

```python
import math
import jax
import jax.numpy as jnp
from jax import lax

MODEL_DIM = 8192
QUERY_HEADS = 64
KEY_VALUE_HEADS = 8
HEAD_SIZE = 128
ROWS_PER_SHARD = 4
NEW_TOKENS = 4
BATCH_ROWS = 32
CACHE_CAPACITY = 512
TOKENS = 128
N_GROUP = 2


def joint_draw(key):
    query_key, cache_draw_key = jax.random.split(jax.random.fold_in(key, 17))
    key_cache_rows = jnp.clip(jax.random.normal(cache_draw_key, (BATCH_ROWS, KEY_VALUE_HEADS, CACHE_CAPACITY, HEAD_SIZE), jnp.float32), -4.0, 4.0)
    query_all = jnp.clip(2.5 * jax.random.normal(query_key, (BATCH_ROWS, NEW_TOKENS, QUERY_HEADS, HEAD_SIZE), jnp.float32), -10.0, 10.0)
    return (query_all.reshape(BATCH_ROWS, NEW_TOKENS, QUERY_HEADS * HEAD_SIZE), key_cache_rows)


def draw_queries(key, part):
    return joint_draw(key)[0].astype(jnp.bfloat16)


def draw_keys(key, part):
    return joint_draw(key)[1].astype(jnp.bfloat16)


def touch_ends(values, key, least, largest):
    place = [jax.random.randint(jax.random.fold_in(key, axis), (), 0, length) for axis, length in enumerate(values.shape)]
    longest = values.shape.index(max(values.shape))
    neighbour = place[:longest] + [(place[longest] + 1) % values.shape[longest]] + place[longest + 1:]
    return values.at[tuple(place)].set(least).at[tuple(neighbour)].set(largest)


def block_levels(stream_key, extent, shards, least, largest):
    loudness = 1.0
    for axis_at, parts in shards:
        steps = jax.random.uniform(jax.random.fold_in(jax.random.fold_in(stream_key, 6), axis_at), (parts,), jnp.float32, least / len(shards), largest / len(shards))
        loudness = loudness * jnp.repeat(jnp.exp(steps), extent[axis_at] // parts).reshape((-1,) + (1,) * (len(extent) - 1 - axis_at))
    return loudness


def normal_values(rng, shape, scale, most, cuts=(), kind=jnp.bfloat16):
    entries = jax.random.normal(rng, shape, jnp.float32) * scale
    if len(cuts) > 0:
        entries = block_levels(rng, shape, cuts, -0.22, 0.18) * entries
    return jnp.clip(entries, min=-most, max=most).astype(kind)


def setup_inputs(seed: int = 0) -> dict:
    key_of = jax.random.split(jax.random.key(seed), 6)
    return {
        "queries": draw_queries(jax.random.fold_in(key_of[5], 71), 0),
        "keys": draw_keys(jax.random.fold_in(key_of[5], 71), 0),
        "values": normal_values(key_of[2], (BATCH_ROWS, KEY_VALUE_HEADS, CACHE_CAPACITY, HEAD_SIZE), 2.0, 12.0, ((0, 8), (2, 4))),
        "cached_length": touch_ends(jax.random.randint(key_of[3], (BATCH_ROWS,), 2, CACHE_CAPACITY - NEW_TOKENS + 1), jax.random.fold_in(key_of[3], 1), 2, CACHE_CAPACITY - NEW_TOKENS).astype(jnp.int32),
        "out_weight": normal_values(key_of[4], (MODEL_DIM, MODEL_DIM), MODEL_DIM ** -0.5, 0.0625, ((0, 4), (1, 8))),
    }


def attend_row_block(inputs):
    query_matrix, key_rows, value_rows, length_rows = inputs
    batch_row_count = query_matrix.shape[0]
    heads_per_group = QUERY_HEADS // KEY_VALUE_HEADS
    reshaped_output = query_matrix.astype(jnp.float32).reshape(batch_row_count, NEW_TOKENS, KEY_VALUE_HEADS, heads_per_group, HEAD_SIZE)
    scores = jnp.einsum('rsgjd,rgpd->rgsjp', reshaped_output, key_rows.astype(jnp.float32)) / math.sqrt(HEAD_SIZE)
    position = jnp.arange(CACHE_CAPACITY, dtype=jnp.int32)
    horizon = length_rows[:, None] + jnp.arange(NEW_TOKENS, dtype=jnp.int32)[None, :] + 1
    allowed = position[None, None, None, None, :] < horizon[:, None, :, None, None]
    masked = jnp.where(allowed, scores, -1e+30)
    row_top = lax.optimization_barrier(jnp.max(masked, axis=-1, keepdims=True))
    exponent = jnp.where(allowed, jnp.exp(masked - row_top), 0.0)
    totals = lax.optimization_barrier(jnp.sum(exponent, axis=-1))
    rounded = lax.optimization_barrier(exponent.astype(jnp.bfloat16)).astype(jnp.float32)
    weighted = jnp.einsum('rgsjp,rgpd->rsgjd', rounded, value_rows.astype(jnp.float32))
    attended_output = weighted / jnp.transpose(totals, (0, 2, 1, 3))[..., None]
    return attended_output.reshape(batch_row_count, NEW_TOKENS, MODEL_DIM).astype(jnp.bfloat16)

def reference(queries, keys, values, cached_length, out_weight):
    row_blocks = BATCH_ROWS // ROWS_PER_SHARD
    attended_output = lax.map(attend_row_block, (queries.reshape(row_blocks, ROWS_PER_SHARD, NEW_TOKENS, MODEL_DIM), keys.reshape(row_blocks, ROWS_PER_SHARD, KEY_VALUE_HEADS, CACHE_CAPACITY, HEAD_SIZE), values.reshape(row_blocks, ROWS_PER_SHARD, KEY_VALUE_HEADS, CACHE_CAPACITY, HEAD_SIZE), cached_length.reshape(row_blocks, ROWS_PER_SHARD)))
    attended_output = attended_output.reshape(TOKENS, MODEL_DIM)
    projected = jnp.dot(attended_output, out_weight, preferred_element_type=jnp.float32).astype(jnp.bfloat16)
    return projected.reshape(TOKENS, N_GROUP, MODEL_DIM // N_GROUP)
```

```python
import functools
import math

import jax
import jax.numpy as jnp
from jax import lax
from jax.experimental import pallas as pl
from jax.experimental.pallas import tpu as pltpu
from jax.sharding import PartitionSpec as P

F32, BF16 = jnp.float32, jnp.bfloat16
LANES, SUBLANES = 128, 8
MASKED = -1e30
PARTS = 3


def vmem(shape, dtype):
    return jax.ShapeDtypeStruct(shape, dtype)


def whole(n):
    return [pl.BlockSpec(memory_space=pltpu.VMEM)] * n


def split3(x):
    hi = x.astype(BF16)
    rest = x - hi.astype(F32)
    mid = rest.astype(BF16)
    return hi, mid, (rest - mid.astype(F32)).astype(BF16)


def pack_stats(m, l, heads):
    lane = lax.broadcasted_iota(jnp.int32, m.shape, 1)
    out = jnp.zeros(m.shape, F32)
    for i, part in enumerate(split3(m) + split3(l)):
        term = jnp.where(lane < heads, part.astype(F32), 0.0)
        out = out + (pltpu.roll(term, i * heads, 1) if i else term)
    return out.astype(BF16)


def unpack_stats(packed, heads):
    x = packed.astype(F32)
    lane = lax.broadcasted_iota(jnp.int32, x.shape, 1)

    def term(i):
        return pltpu.roll(x, LANES - i * heads, 1) if i else x

    m = (term(0) + term(1)) + term(2)
    l = (term(3) + term(4)) + term(5)
    return jnp.where(lane < heads, m, 0.0), jnp.where(lane < heads, l, 0.0)


def attention_kernel(heads, join, len_ref, q_ref, k_ref, v_ref, send_ref, acc_ref, stat_ref, q_scr, o_scr, s_scr):
    rows, steps, _ = q_ref.shape
    cache, dim = k_ref.shape[2:]
    q_heads = q_ref.shape[2] // dim
    per_kv = q_heads // k_ref.shape[1]
    tensor = q_heads // heads
    width = heads * dim
    me = lax.axis_index("tensor")
    scale = 1.0 / math.sqrt(dim)
    shape = (join * steps, cache)
    row = lax.broadcasted_iota(jnp.int32, shape, 0)
    position = me * cache + lax.broadcasted_iota(jnp.int32, shape, 1) - row % steps
    lane = lax.broadcasted_iota(jnp.int32, (join * steps, LANES), 1)
    srow = lax.broadcasted_iota(jnp.int32, (join * steps, LANES), 0)
    for chunk in range(tensor):
        owner = me ^ chunk
        for part in range(heads // join):
            head = owner * heads + part * join
            kv = head // per_kv
            for r in range(rows):
                slot = (chunk * (heads // join) + part) * rows + r
                for j in range(join):
                    q_scr[slot, pl.ds(j * steps, steps), :] = q_ref[
                        r, :, pl.ds(pl.multiple_of((head + j) * dim, dim), dim)
                    ].astype(F32)
                q = q_scr[slot].astype(BF16)
                s = lax.dot_general(
                    q, k_ref[r, kv], (((1,), (1,)), ((), ())), preferred_element_type=F32
                ) * scale
                allowed = position < len_ref[r] + 1
                s = jnp.where(allowed, s, MASKED)
                m = jnp.max(s, axis=1, keepdims=True)
                p = jnp.where(allowed, jnp.exp(s - m), 0.0)
                l = jnp.sum(p, axis=1, keepdims=True)
                o = jnp.dot(p.astype(BF16), v_ref[r, kv], preferred_element_type=F32)
                tokens = pl.ds(r * steps, steps)
                for j in range(join):
                    o_scr[chunk, tokens, pl.ds((part * join + j) * dim, dim)] = o[j * steps : (j + 1) * steps]
                for i, stat in enumerate((m, l)):
                    x = jnp.where(lane == part * join + srow // steps, stat, 0.0)
                    total = x[:SUBLANES]
                    for b in range(SUBLANES, join * steps, SUBLANES):
                        total = total + x[b : b + SUBLANES]
                    shift = steps
                    while shift < SUBLANES:
                        total = total + pltpu.roll(total, shift, 0)
                        shift *= 2
                    if part:
                        s_scr[chunk, i, tokens, :] += total[:steps]
                    else:
                        s_scr[chunk, i, tokens, :] = total[:steps]
        half = chunk // 2
        if chunk % 2:
            send_ref[half, :, pl.ds(0, width)] = o_scr[chunk].astype(BF16)
            send_ref[half, :, pl.ds(width, LANES)] = pack_stats(s_scr[chunk, 0], s_scr[chunk, 1], heads)
        else:
            acc_ref[half] = o_scr[chunk]
            stat_ref[half] = s_scr[chunk]


def attention(queries, keys, values, lengths, tensor):
    rows, steps, model = queries.shape
    kv_heads, dim = keys.shape[1], keys.shape[3]
    q_heads = model // dim
    heads = q_heads // tensor
    join = min(heads, q_heads // kv_heads)
    width, tokens, halves = heads * dim, rows * steps, tensor // 2
    return pl.pallas_call(
        functools.partial(attention_kernel, heads, join),
        out_shape=(
            vmem((halves, tokens, width + LANES), BF16),
            vmem((halves, tokens, width), F32),
            vmem((halves, 2, tokens, LANES), F32),
        ),
        in_specs=[pl.BlockSpec(memory_space=pltpu.SMEM)] + whole(3),
        out_specs=whole(3),
        scratch_shapes=[
            pltpu.VMEM((rows * q_heads // join, join * steps, dim), F32),
            pltpu.VMEM((tensor, tokens, width), F32),
            pltpu.VMEM((tensor, 2, tokens, LANES), F32),
        ],
        name="attention",
    )(lengths, queries, keys, values)


def merged(acc, m, l, received, heads):
    width = acc.shape[1]
    dim = width // heads
    m2, l2 = unpack_stats(received[:, width:], heads)
    top = jnp.maximum(m, m2)
    e1, e2 = jnp.exp(m - top), jnp.exp(m2 - top)
    columns = [
        e1[:, i : i + 1] * acc[:, i * dim : (i + 1) * dim]
        + e2[:, i : i + 1] * received[:, i * dim : (i + 1) * dim].astype(F32)
        for i in range(heads)
    ]
    return columns, top, e1 * l + e2 * l2


def core_merge_kernel(heads, acc_ref, stat_ref, recv_ref, send_ref, own_ref, own_stat_ref):
    width = acc_ref.shape[2]
    dim = width // heads
    for k in range(acc_ref.shape[0]):
        columns, m, l = merged(acc_ref[k], stat_ref[k, 0], stat_ref[k, 1], recv_ref[k], heads)
        for i, c in enumerate(columns):
            if k:
                send_ref[k - 1, :, pl.ds(i * dim, dim)] = c.astype(BF16)
            else:
                own_ref[:, pl.ds(i * dim, dim)] = c
        if k:
            send_ref[k - 1, :, pl.ds(width, LANES)] = pack_stats(m, l, heads)
        else:
            own_stat_ref[0] = m
            own_stat_ref[1] = l


def core_merge(acc, stat, received, heads):
    halves, tokens, width = acc.shape
    return pl.pallas_call(
        functools.partial(core_merge_kernel, heads),
        out_shape=(
            vmem((halves - 1, tokens, width + LANES), BF16),
            vmem((tokens, width), F32),
            vmem((2, tokens, LANES), F32),
        ),
        in_specs=whole(3),
        out_specs=whole(3),
        name="core_merge",
    )(acc, stat, received)


def final_merge_kernel(heads, n, own_ref, stat_ref, *refs):
    recv, out_ref = refs[:n], refs[n]
    width = own_ref.shape[1]
    dim = width // heads
    acc, m, l = own_ref[...], stat_ref[0], stat_ref[1]
    for i, r in enumerate(recv):
        columns, m, l = merged(acc, m, l, r[...], heads)
        acc = jnp.concatenate(columns, axis=1)
    inverse = 1.0 / l
    for i in range(heads):
        out_ref[:, pl.ds(i * dim, dim)] = (
            acc[:, i * dim : (i + 1) * dim] * inverse[:, i : i + 1]
        ).astype(BF16)


def final_merge(own, stat, received, heads):
    return pl.pallas_call(
        functools.partial(final_merge_kernel, heads, len(received)),
        out_shape=vmem(own.shape, BF16),
        in_specs=whole(2 + len(received)),
        out_specs=pl.BlockSpec(memory_space=pltpu.VMEM),
        name="final_merge",
    )(own, stat, *received)


def project_kernel(groups, dps, halves, *refs):
    blocks, w_ref = refs[: groups * dps], refs[groups * dps]
    send_ref, keep_ref, lhs = refs[groups * dps + 1 :]
    tokens = blocks[0].shape[0]
    twist = lax.axis_index("dp") ^ lax.axis_index("tensor")
    for kg in range(groups):
        for kd in range(dps):
            at = kg * dps + (twist ^ kd)
            lhs[pl.ds(pl.multiple_of(at * tokens, tokens), tokens), :] = blocks[kg * dps + kd][...]
    out = jnp.dot(lhs[...], w_ref[...], preferred_element_type=F32)
    for kg in range(groups):
        for kt in range(2 * halves):
            piece = out[(kg * dps + kt) * tokens : (kg * dps + kt + 1) * tokens]
            if kt % 2:
                send_ref[kg, kt // 2] = piece.astype(BF16)
            else:
                keep_ref[kg, kt // 2] = piece


def project(blocks, weight, groups, dps, halves):
    tokens, width = blocks[0].shape
    columns = weight.shape[1]
    shape = (groups, halves, tokens, columns)
    return pl.pallas_call(
        functools.partial(project_kernel, groups, dps, halves),
        out_shape=(vmem(shape, BF16), vmem(shape, F32)),
        in_specs=whole(len(blocks) + 1),
        out_specs=whole(2),
        scratch_shapes=[pltpu.VMEM((groups * dps * tokens, width), BF16)],
        name="project",
    )(*blocks, weight)


def swap(x, axes, n, k):
    return lax.ppermute(x, axes, [(i, i ^ k) for i in range(n)])


def on_device(queries, keys, values, cached_length, out_weight):
    rows, steps, model = queries.shape
    q_heads = model // keys.shape[3]
    tensor, groups, dps = lax.axis_size("tensor"), lax.axis_size("group"), lax.axis_size("dp")
    halves, heads, tokens = tensor // 2, q_heads // tensor, rows * steps

    send, acc, stat = attention(queries, keys, values, cached_length, tensor)
    send, own, stat = core_merge(acc, stat, swap(send, "tensor", tensor, 1), heads)
    arrived = [swap(send[k - 1], "tensor", tensor, 2 * k) for k in range(1, halves)]
    attended = final_merge(own, stat, arrived, heads)

    line = [attended] + [swap(attended, "dp", dps, k) for k in range(1, dps)]
    blocks = list(line)
    for kg in range(1, groups):
        blocks += [swap(b, "group", groups, kg) for b in line]
    send, keep = project(blocks, out_weight, groups, dps, halves)

    both = keep + swap(send, "tensor", tensor, 1).astype(F32)
    plane, n = ("group", "tensor"), groups * tensor
    sums = []
    for kg in range(groups):
        total = both[0, 0] if kg == 0 else 0.0
        for kx in range(halves):
            if kg or kx:
                total = total + swap(both[kg, kx].astype(BF16), plane, n, kg * tensor + 2 * kx).astype(F32)
        sums.append(total)
    me = lax.axis_index("group")
    placed = []
    for g in range(groups):
        kept = sums[0]
        for kg in range(1, groups):
            kept = jnp.where(me ^ kg == g, sums[kg], kept)
        placed.append(kept)
    return jnp.stack(placed, axis=1).astype(BF16)


def solution(mesh):
    in_specs = (
        P(("group", "dp"), None, None),
        P(("group", "dp"), None, "tensor", None),
        P(("group", "dp"), None, "tensor", None),
        P(("group", "dp")),
        P("tensor", ("group", "dp")),
    )
    out_specs = P(("group", "tensor"), None, "dp")
    return jax.shard_map(
        on_device, mesh=mesh, in_specs=in_specs, out_specs=out_specs, check_vma=False
    )
```

```python
import functools
import math

import jax
import jax.numpy as jnp
from jax import lax
from jax.experimental import pallas as pl
from jax.experimental.pallas import tpu as pltpu
from jax.sharding import PartitionSpec as P


F32, BF16 = jnp.float32, jnp.bfloat16
LANES, SUBLANES = 128, 8
MASKED = -1e30
FETCH_FLOPS = 1 << 27


def vmem(shape, dtype):
    return pltpu.VMEM(shape, dtype)


def whole(n):
    return [pl.BlockSpec(memory_space=pltpu.VMEM)] * n


def held(*arrays):
    return [pltpu.with_memory_space_constraint(x, pltpu.VMEM) for x in arrays]


def in_hbm(*arrays):
    return [pltpu.with_memory_space_constraint(x, pltpu.HBM) for x in arrays]


def fetch_kernel(_, w_hbm, w_ref, sem):
    copy = pltpu.make_async_copy(w_hbm, w_ref, sem)
    copy.start()
    copy.wait()


def fetch(after, weight):
    return pl.pallas_call(
        fetch_kernel,
        out_shape=vmem(weight.shape, weight.dtype),
        in_specs=[pl.BlockSpec(memory_space=pltpu.VMEM), pl.BlockSpec(memory_space=pltpu.HBM)],
        out_specs=pl.BlockSpec(memory_space=pltpu.VMEM),
        scratch_shapes=[pltpu.SemaphoreType.DMA],
        cost_estimate=pl.CostEstimate(flops=FETCH_FLOPS, bytes_accessed=weight.size * 2, transcendentals=0),
        compiler_params=pltpu.CompilerParams(vmem_limit_bytes=1 << 20),
        name="fetch",
    )(*held(after), *in_hbm(weight))


def split3(x):
    hi = x.astype(BF16)
    rest = x - hi.astype(F32)
    mid = rest.astype(BF16)
    return hi, mid, (rest - mid.astype(F32)).astype(BF16)


def pack_stats(m, l, heads):
    lane = lax.broadcasted_iota(jnp.int32, m.shape, 1)
    out = jnp.zeros(m.shape, F32)
    for i, part in enumerate(split3(m) + split3(l)):
        term = jnp.where(lane < heads, part.astype(F32), 0.0)
        out = out + (pltpu.roll(term, i * heads, 1) if i else term)
    return out.astype(BF16)


def unpack_stats(packed, heads):
    x = packed.astype(F32)
    lane = lax.broadcasted_iota(jnp.int32, x.shape, 1)

    def term(i):
        return pltpu.roll(x, LANES - i * heads, 1) if i else x

    m = (term(0) + term(1)) + term(2)
    l = (term(3) + term(4)) + term(5)
    return jnp.where(lane < heads, m, 0.0), jnp.where(lane < heads, l, 0.0)


def attention_kernel(heads, join, len_hbm, q_hbm, k_hbm, v_hbm, send_ref, acc_ref, stat_ref, len_scr, q_scr, k_scr, v_scr, f_scr, o_scr, s_scr, sems):
    rows, steps, model = q_hbm.shape
    kv_heads, cache, dim = k_hbm.shape[1:]
    q_heads = model // dim
    per_kv = q_heads // kv_heads
    tensor, width, parts, span = q_heads // heads, heads * dim, heads // join, k_scr.shape[2]
    me = lax.axis_index("tensor")
    order = list(range(1, tensor, 2)) + list(range(0, tensor, 2))
    copies = []
    for chunk in range(tensor):
        owner = me ^ chunk
        kv = owner * heads // per_kv
        copies.append([
            pltpu.make_async_copy(q_hbm.at[:, :, pl.ds(pl.multiple_of(owner * width, width), width)], q_scr.at[chunk], sems.at[0, chunk]),
            pltpu.make_async_copy(k_hbm.at[:, pl.ds(kv, span)], k_scr.at[chunk], sems.at[1, chunk]),
            pltpu.make_async_copy(v_hbm.at[:, pl.ds(kv, span)], v_scr.at[chunk], sems.at[2, chunk]),
        ])
    limits = pltpu.make_async_copy(len_hbm, len_scr, sems.at[3, 0])
    limits.start()
    for chunk in order:
        for copy in copies[chunk]:
            copy.start()
    limits.wait()
    scale = 1.0 / math.sqrt(dim)
    m_rows = join * steps
    row = lax.broadcasted_iota(jnp.int32, (m_rows, cache), 0)
    position = me * cache + lax.broadcasted_iota(jnp.int32, (m_rows, cache), 1) - row % steps
    lane = lax.broadcasted_iota(jnp.int32, (m_rows, LANES), 1)
    srow = lax.broadcasted_iota(jnp.int32, (m_rows, LANES), 0)
    allowed = [position < len_scr[r] + 1 for r in range(rows)]
    for chunk in order:
        units = [(part, r) for part in range(parts) for r in range(rows)]
        copies[chunk][0].wait()
        for u, (part, r) in enumerate(units):
            for j in range(join):
                f_scr[chunk, u, pl.ds(j * steps, steps), :] = q_scr[chunk, r, :, pl.ds((part * join + j) * dim, dim)].astype(F32)
        copies[chunk][1].wait()
        s = [
            lax.dot_general(
                f_scr[chunk, u].astype(BF16), k_scr[chunk, r, part * span // parts],
                (((1,), (1,)), ((), ())), preferred_element_type=F32,
            )
            for u, (part, r) in enumerate(units)
        ]
        s = [jnp.where(allowed[r], x * scale, MASKED) for x, (_, r) in zip(s, units)]
        m = [jnp.max(x, axis=1, keepdims=True) for x in s]
        p = [jnp.where(allowed[r], jnp.exp(x - y), 0.0) for x, y, (_, r) in zip(s, m, units)]
        l = [jnp.sum(x, axis=1, keepdims=True) for x in p]
        copies[chunk][2].wait()
        o = [
            jnp.dot(x.astype(BF16), v_scr[chunk, r, part * span // parts], preferred_element_type=F32)
            for x, (part, r) in zip(p, units)
        ]
        for x, (part, r) in zip(o, units):
            for j in range(join):
                o_scr[chunk, pl.ds(r * steps, steps), pl.ds((part * join + j) * dim, dim)] = x[j * steps : (j + 1) * steps]
        for i, stat in enumerate((m, l)):
            for r in range(rows):
                total = 0.0
                for x, (part, at) in zip(stat, units):
                    if at == r:
                        x = jnp.where(lane == part * join + srow // steps, x, 0.0)
                        for b in range(0, m_rows, SUBLANES):
                            total = total + x[b : b + SUBLANES]
                shift = steps
                while shift < SUBLANES:
                    total = total + pltpu.roll(total, shift, 0)
                    shift *= 2
                s_scr[chunk, i, pl.ds(r * steps, steps), :] = total[:steps]
        half = chunk // 2
        if chunk % 2:
            send_ref[half, :, pl.ds(0, width)] = o_scr[chunk].astype(BF16)
            send_ref[half, :, pl.ds(width, LANES)] = pack_stats(s_scr[chunk, 0], s_scr[chunk, 1], heads)
        else:
            acc_ref[half] = o_scr[chunk]
            stat_ref[half] = s_scr[chunk]


def attention(queries, keys, values, lengths, tensor):
    rows, steps, model = queries.shape
    kv_heads, cache, dim = keys.shape[1:]
    q_heads = model // dim
    heads = q_heads // tensor
    per_kv = q_heads // kv_heads
    join, span = min(heads, per_kv), max(1, heads // per_kv)
    width, tokens, halves = heads * dim, rows * steps, tensor // 2
    return pl.pallas_call(
        functools.partial(attention_kernel, heads, join),
        out_shape=(
            vmem((halves, tokens, width + LANES), BF16),
            vmem((halves, tokens, width), F32),
            vmem((halves, 2, tokens, LANES), F32),
        ),
        in_specs=[pl.BlockSpec(memory_space=pltpu.HBM)] * 4,
        out_specs=whole(3),
        scratch_shapes=[
            pltpu.SMEM((rows,), jnp.int32),
            pltpu.VMEM((tensor, rows, steps, width), BF16),
            pltpu.VMEM((tensor, rows, span, cache, dim), BF16),
            pltpu.VMEM((tensor, rows, span, cache, dim), BF16),
            pltpu.VMEM((tensor, rows * heads // join, join * steps, dim), F32),
            pltpu.VMEM((tensor, tokens, width), F32),
            pltpu.VMEM((tensor, 2, tokens, LANES), F32),
            pltpu.SemaphoreType.DMA((4, tensor)),
        ],
        compiler_params=pltpu.CompilerParams(vmem_limit_bytes=16 << 20),
        name="attention",
    )(*in_hbm(lengths, queries, keys, values))


def merged(acc, m, l, received, heads):
    width = acc.shape[1]
    dim = width // heads
    m2, l2 = unpack_stats(received[:, width:], heads)
    top = jnp.maximum(m, m2)
    e1, e2 = jnp.exp(m - top), jnp.exp(m2 - top)
    columns = [
        e1[:, i : i + 1] * acc[:, i * dim : (i + 1) * dim]
        + e2[:, i : i + 1] * received[:, i * dim : (i + 1) * dim].astype(F32)
        for i in range(heads)
    ]
    return columns, top, e1 * l + e2 * l2


def core_merge_kernel(heads, acc_ref, stat_ref, recv_ref, send_ref, own_ref, own_stat_ref):
    width = acc_ref.shape[2]
    dim = width // heads
    for k in range(acc_ref.shape[0]):
        columns, m, l = merged(acc_ref[k], stat_ref[k, 0], stat_ref[k, 1], recv_ref[k], heads)
        for i, c in enumerate(columns):
            if k:
                send_ref[k - 1, :, pl.ds(i * dim, dim)] = c.astype(BF16)
            else:
                own_ref[:, pl.ds(i * dim, dim)] = c
        if k:
            send_ref[k - 1, :, pl.ds(width, LANES)] = pack_stats(m, l, heads)
        else:
            own_stat_ref[0] = m
            own_stat_ref[1] = l


def core_merge(acc, stat, received, heads):
    halves, tokens, width = acc.shape
    return pl.pallas_call(
        functools.partial(core_merge_kernel, heads),
        out_shape=(
            vmem((halves - 1, tokens, width + LANES), BF16),
            vmem((tokens, width), F32),
            vmem((2, tokens, LANES), F32),
        ),
        in_specs=whole(3),
        out_specs=whole(3),
        compiler_params=pltpu.CompilerParams(vmem_limit_bytes=8 << 20),
        name="core_merge",
    )(*held(acc, stat, received))


def final_merge_kernel(heads, n, own_ref, stat_ref, *refs):
    recv, out_ref = refs[:n], refs[n]
    width = own_ref.shape[1]
    dim = width // heads
    acc, m, l = own_ref[...], stat_ref[0], stat_ref[1]
    for r in recv:
        columns, m, l = merged(acc, m, l, r[...], heads)
        acc = jnp.concatenate(columns, axis=1)
    inverse = 1.0 / l
    for i in range(heads):
        out_ref[:, pl.ds(i * dim, dim)] = (
            acc[:, i * dim : (i + 1) * dim] * inverse[:, i : i + 1]
        ).astype(BF16)


def final_merge(own, stat, received, heads):
    return pl.pallas_call(
        functools.partial(final_merge_kernel, heads, len(received)),
        out_shape=vmem(own.shape, BF16),
        in_specs=whole(2 + len(received)),
        out_specs=pl.BlockSpec(memory_space=pltpu.VMEM),
        compiler_params=pltpu.CompilerParams(vmem_limit_bytes=8 << 20),
        name="final_merge",
    )(*held(own, stat, *received))


def project_kernel(groups, dps, halves, *refs):
    blocks, w_ref = refs[: groups * dps], refs[groups * dps]
    send_ref, keep_ref, lhs = refs[groups * dps + 1 :]
    tokens = blocks[0].shape[0]
    twist = lax.axis_index("dp") ^ lax.axis_index("tensor")
    for kg in range(groups):
        for kd in range(dps):
            at = kg * dps + (twist ^ kd)
            lhs[pl.ds(pl.multiple_of(at * tokens, tokens), tokens), :] = blocks[kg * dps + kd][...]
    out = jnp.dot(lhs[...], w_ref[...], preferred_element_type=F32)
    for kg in range(groups):
        for kt in range(2 * halves):
            piece = out[(kg * dps + kt) * tokens : (kg * dps + kt + 1) * tokens]
            if kt % 2:
                send_ref[kg, kt // 2] = piece.astype(BF16)
            else:
                keep_ref[kg, kt // 2] = piece


def project(blocks, weight, groups, dps, halves):
    tokens, width = blocks[0].shape
    columns = weight.shape[1]
    shape = (groups, halves, tokens, columns)
    return pl.pallas_call(
        functools.partial(project_kernel, groups, dps, halves),
        out_shape=(vmem(shape, BF16), vmem(shape, F32)),
        in_specs=whole(len(blocks) + 1),
        out_specs=whole(2),
        scratch_shapes=[pltpu.VMEM((groups * dps * tokens, width), BF16)],
        compiler_params=pltpu.CompilerParams(vmem_limit_bytes=16 << 20),
        name="project",
    )(*held(*blocks, weight))


def swap(x, axes, n, k):
    return lax.ppermute(x, axes, [(i, i ^ k) for i in range(n)])


def on_device(queries, keys, values, cached_length, out_weight):
    _, _, model = queries.shape
    q_heads = model // keys.shape[3]
    tensor, groups, dps = lax.axis_size("tensor"), lax.axis_size("group"), lax.axis_size("dp")
    halves, heads = tensor // 2, q_heads // tensor

    send, acc, stat = attention(queries, keys, values, cached_length, tensor)
    send, own, stat = core_merge(acc, stat, swap(send, "tensor", tensor, 1), heads)
    weight = fetch(stat, out_weight)
    arrived = [swap(send[k - 1], "tensor", tensor, 2 * k) for k in range(1, halves)]
    attended = final_merge(own, stat, arrived, heads)

    line = [attended]
    for k in range(1, dps):
        line.append(swap(attended, "dp", dps, k))
    blocks = list(line)
    for kg in range(1, groups):
        for b in line:
            blocks.append(swap(b, "group", groups, kg))
    send, keep = project(blocks, weight, groups, dps, halves)

    both = keep + swap(send, "tensor", tensor, 1).astype(F32)
    plane, n = ("group", "tensor"), groups * tensor
    sums = []
    for kg in range(groups):
        total = both[0, 0] if kg == 0 else 0.0
        for kx in range(halves):
            if kg or kx:
                total = total + swap(both[kg, kx].astype(BF16), plane, n, kg * tensor + 2 * kx).astype(F32)
        sums.append(total)
    me = lax.axis_index("group")
    placed = []
    for g in range(groups):
        kept = sums[0]
        for kg in range(1, groups):
            kept = jnp.where(me ^ kg == g, sums[kg], kept)
        placed.append(kept)
    return jnp.stack(placed, axis=1).astype(BF16)


def solution(mesh):
    in_specs = (
        P(("group", "dp"), None, None),
        P(("group", "dp"), None, "tensor", None),
        P(("group", "dp"), None, "tensor", None),
        P(("group", "dp")),
        P("tensor", ("group", "dp")),
    )
    out_specs = P(("group", "tensor"), None, "dp")
    return jax.shard_map(
        on_device, mesh=mesh, in_specs=in_specs, out_specs=out_specs, check_vma=False
    )
```

```python
import functools
import math

import jax
import jax.numpy as jnp
from jax import lax
from jax.experimental import pallas as pl
from jax.experimental.pallas import tpu as pltpu
from jax.sharding import PartitionSpec as P


F32, BF16 = jnp.float32, jnp.bfloat16
LANES, SUBLANES = 128, 8
MASKED = -1e30
FETCH_FLOPS = 1 << 27


def vmem(shape, dtype):
    return pltpu.VMEM(shape, dtype)


def whole(n):
    return [pl.BlockSpec(memory_space=pltpu.VMEM)] * n


def held(*arrays):
    return [pltpu.with_memory_space_constraint(x, pltpu.VMEM) for x in arrays]


def in_hbm(*arrays):
    return [pltpu.with_memory_space_constraint(x, pltpu.HBM) for x in arrays]


def fetch_kernel(_, w_hbm, w_ref, sem):
    copy = pltpu.make_async_copy(w_hbm, w_ref, sem)
    copy.start()
    copy.wait()


def fetch(after, weight):
    return pl.pallas_call(
        fetch_kernel,
        out_shape=vmem(weight.shape, weight.dtype),
        in_specs=[pl.BlockSpec(memory_space=pltpu.VMEM), pl.BlockSpec(memory_space=pltpu.HBM)],
        out_specs=pl.BlockSpec(memory_space=pltpu.VMEM),
        scratch_shapes=[pltpu.SemaphoreType.DMA],
        cost_estimate=pl.CostEstimate(flops=FETCH_FLOPS, bytes_accessed=weight.size * 2, transcendentals=0),
        compiler_params=pltpu.CompilerParams(vmem_limit_bytes=1 << 20),
        name="fetch",
    )(*held(after), *in_hbm(weight))


def split3(x):
    hi = x.astype(BF16)
    rest = x - hi.astype(F32)
    mid = rest.astype(BF16)
    return hi, mid, (rest - mid.astype(F32)).astype(BF16)


def pack_stats(m, l, heads):
    lane = lax.broadcasted_iota(jnp.int32, m.shape, 1)
    out = jnp.zeros(m.shape, F32)
    for i, part in enumerate(split3(m) + split3(l)):
        term = jnp.where(lane < heads, part.astype(F32), 0.0)
        out = out + (pltpu.roll(term, i * heads, 1) if i else term)
    return out.astype(BF16)


def unpack_stats(packed, heads):
    x = packed.astype(F32)
    lane = lax.broadcasted_iota(jnp.int32, x.shape, 1)

    def term(i):
        return pltpu.roll(x, LANES - i * heads, 1) if i else x

    m = (term(0) + term(1)) + term(2)
    l = (term(3) + term(4)) + term(5)
    return jnp.where(lane < heads, m, 0.0), jnp.where(lane < heads, l, 0.0)


def attend(heads, join, q_ref, k_ref, v_ref, gap_ref, f_scr, o_ref, s_ref):
    rows, steps, _ = q_ref.shape
    span, _, dim = k_ref.shape[1:]
    parts, m_rows = heads // join, join * steps
    scale = 1.0 / math.sqrt(dim)
    lane = lax.broadcasted_iota(jnp.int32, (m_rows, LANES), 1)
    srow = lax.broadcasted_iota(jnp.int32, (m_rows, LANES), 0)
    allowed = [gap_ref[r] < 1 for r in range(rows)]
    units = [(part, r) for part in range(parts) for r in range(rows)]
    for u, (part, r) in enumerate(units):
        for j in range(join):
            f_scr[u, pl.ds(j * steps, steps), :] = q_ref[r, :, pl.ds((part * join + j) * dim, dim)].astype(F32)
    s = [
        lax.dot_general(
            f_scr[u].astype(BF16), k_ref[r, part * span // parts],
            (((1,), (1,)), ((), ())), preferred_element_type=F32,
        )
        for u, (part, r) in enumerate(units)
    ]
    s = [jnp.where(allowed[r], x * scale, MASKED) for x, (_, r) in zip(s, units)]
    m = [jnp.max(x, axis=1, keepdims=True) for x in s]
    p = [jnp.where(allowed[r], jnp.exp(x - y), 0.0) for x, y, (_, r) in zip(s, m, units)]
    l = [jnp.sum(x, axis=1, keepdims=True) for x in p]
    o = [
        jnp.dot(x.astype(BF16), v_ref[r, part * span // parts], preferred_element_type=F32)
        for x, (part, r) in zip(p, units)
    ]
    for x, (part, r) in zip(o, units):
        for j in range(join):
            o_ref[pl.ds(r * steps, steps), pl.ds((part * join + j) * dim, dim)] = x[j * steps : (j + 1) * steps]
    for i, stat in enumerate((m, l)):
        for r in range(rows):
            total = 0.0
            for x, (part, at) in zip(stat, units):
                if at == r:
                    x = jnp.where(lane == part * join + srow // steps, x, 0.0)
                    for b in range(0, m_rows, SUBLANES):
                        total = total + x[b : b + SUBLANES]
            shift = steps
            while shift < SUBLANES:
                total = total + pltpu.roll(total, shift, 0)
                shift *= 2
            s_ref[i, pl.ds(r * steps, steps), :] = total[:steps]


def attend_packed(heads, join, q_ref, k_ref, v_ref, gap_ref, f_scr, o_scr, s_scr, send_ref):
    attend(heads, join, q_ref, k_ref, v_ref, gap_ref, f_scr, o_scr, s_scr)
    width = o_scr.shape[1]
    send_ref[:, pl.ds(0, width)] = o_scr[...].astype(BF16)
    send_ref[:, pl.ds(width, LANES)] = pack_stats(s_scr[0], s_scr[1], heads)


def first_kernel(heads, join, chunks, order, len_hbm, q_hbm, k_hbm, v_hbm, send_ref, q_ref, k_ref, v_ref, gap_ref, len_scr, f_scr, o_scr, s_scr, sems):
    rows = q_hbm.shape[0]
    kv_heads, cache, dim = k_hbm.shape[1:]
    q_heads = q_hbm.shape[2] // dim
    tensor, width, span = q_heads // heads, heads * dim, k_ref.shape[2]
    me = lax.axis_index("tensor")
    copies = []
    for chunk in range(tensor):
        owner = me ^ chunk
        kv = owner * heads // (q_heads // kv_heads)
        copies.append([
            pltpu.make_async_copy(q_hbm.at[:, :, pl.ds(pl.multiple_of(owner * width, width), width)], q_ref.at[chunk], sems.at[0, chunk]),
            pltpu.make_async_copy(k_hbm.at[:, pl.ds(kv, span)], k_ref.at[chunk], sems.at[1, chunk]),
            pltpu.make_async_copy(v_hbm.at[:, pl.ds(kv, span)], v_ref.at[chunk], sems.at[2, chunk]),
        ])
    limits = pltpu.make_async_copy(len_hbm, len_scr, sems.at[3, 0])
    limits.start()
    for chunk in order:
        for copy in copies[chunk]:
            copy.start()
    limits.wait()
    shape = gap_ref.shape[1:]
    row = lax.broadcasted_iota(jnp.int32, shape, 0)
    steps = q_hbm.shape[1]
    position = me * cache + lax.broadcasted_iota(jnp.int32, shape, 1) - row % steps
    for r in range(rows):
        gap_ref[r] = position - len_scr[r]
    for i, chunk in enumerate(chunks):
        for copy in copies[chunk]:
            copy.wait()
        attend_packed(heads, join, q_ref.at[chunk], k_ref.at[chunk], v_ref.at[chunk], gap_ref, f_scr.at[i], o_scr.at[i], s_scr.at[i], send_ref.at[i])
    for chunk in order:
        if chunk not in chunks:
            for copy in copies[chunk]:
                copy.wait()


def send_kernel(heads, join, chunk, q_ref, k_ref, v_ref, gap_ref, send_ref, f_scr, o_scr, s_scr):
    attend_packed(heads, join, q_ref.at[chunk], k_ref.at[chunk], v_ref.at[chunk], gap_ref, f_scr, o_scr, s_scr, send_ref)


def keep_kernel(heads, join, chunks, q_ref, k_ref, v_ref, gap_ref, acc_ref, stat_ref, f_scr):
    for i, c in enumerate(chunks):
        attend(heads, join, q_ref.at[c], k_ref.at[c], v_ref.at[c], gap_ref, f_scr.at[i], acc_ref.at[i], stat_ref.at[i])


class Attention:
    def __init__(self, queries, keys, tensor):
        self.rows, self.steps, model = queries.shape
        kv_heads, self.cache, self.dim = keys.shape[1:]
        q_heads = model // self.dim
        per_kv = q_heads // kv_heads
        self.tensor, self.heads = tensor, q_heads // tensor
        self.join, self.span = min(self.heads, per_kv), max(1, self.heads // per_kv)
        self.width, self.tokens = self.heads * self.dim, self.rows * self.steps
        self.m_rows = self.join * self.steps

    def scratch(self, n):
        lead = (n,) if n else ()
        return [
            pltpu.VMEM((*lead, self.rows * self.heads // self.join, self.m_rows, self.dim), F32),
            pltpu.VMEM((*lead, self.tokens, self.width), F32),
            pltpu.VMEM((*lead, 2, self.tokens, LANES), F32),
        ]

    def options(self, n):
        work = 4 * n * self.tokens * self.width * self.cache
        return dict(
            cost_estimate=pl.CostEstimate(flops=4 * work, bytes_accessed=0, transcendentals=0),
            compiler_params=pltpu.CompilerParams(vmem_limit_bytes=8 << 20),
        )

    def first(self, chunks, order, lengths, queries, keys, values):
        cached = (self.tensor, self.rows, self.span, self.cache, self.dim)
        return pl.pallas_call(
            functools.partial(first_kernel, self.heads, self.join, chunks, order),
            out_shape=(
                vmem((len(chunks), self.tokens, self.width + LANES), BF16),
                vmem((self.tensor, self.rows, self.steps, self.width), BF16),
                vmem(cached, BF16),
                vmem(cached, BF16),
                vmem((self.rows, self.m_rows, self.cache), jnp.int32),
            ),
            in_specs=[pl.BlockSpec(memory_space=pltpu.HBM)] * 4,
            out_specs=whole(5),
            scratch_shapes=[pltpu.SMEM((self.rows,), jnp.int32)] + self.scratch(len(chunks)) + [pltpu.SemaphoreType.DMA((4, self.tensor))],
            name="attend_first",
            **self.options(len(chunks)),
        )(*in_hbm(lengths, queries, keys, values))

    def send(self, chunk, *loaded):
        return pl.pallas_call(
            functools.partial(send_kernel, self.heads, self.join, chunk),
            out_shape=vmem((self.tokens, self.width + LANES), BF16),
            in_specs=whole(4),
            out_specs=pl.BlockSpec(memory_space=pltpu.VMEM),
            scratch_shapes=self.scratch(0),
            name="attend_send",
            **self.options(1),
        )(*held(*loaded))

    def keep(self, chunks, *loaded):
        n = len(chunks)
        return pl.pallas_call(
            functools.partial(keep_kernel, self.heads, self.join, chunks),
            out_shape=(vmem((n, self.tokens, self.width), F32), vmem((n, 2, self.tokens, LANES), F32)),
            in_specs=whole(4),
            out_specs=whole(2),
            scratch_shapes=self.scratch(n)[:1],
            name="attend_keep",
            **self.options(n),
        )(*held(*loaded))


def merged(acc, m, l, received, heads):
    width = acc.shape[1]
    dim = width // heads
    m2, l2 = unpack_stats(received[:, width:], heads)
    top = jnp.maximum(m, m2)
    e1, e2 = jnp.exp(m - top), jnp.exp(m2 - top)
    columns = [
        e1[:, i : i + 1] * acc[:, i * dim : (i + 1) * dim]
        + e2[:, i : i + 1] * received[:, i * dim : (i + 1) * dim].astype(F32)
        for i in range(heads)
    ]
    return columns, top, e1 * l + e2 * l2


def core_merge_kernel(heads, acc_ref, stat_ref, recv_ref, send_ref):
    width = acc_ref.shape[2]
    dim = width // heads
    for k in range(acc_ref.shape[0]):
        columns, m, l = merged(acc_ref[k], stat_ref[k, 0], stat_ref[k, 1], recv_ref[k], heads)
        for i, c in enumerate(columns):
            send_ref[k, :, pl.ds(i * dim, dim)] = c.astype(BF16)
        send_ref[k, :, pl.ds(width, LANES)] = pack_stats(m, l, heads)


def core_merge(acc, stat, received, heads):
    return pl.pallas_call(
        functools.partial(core_merge_kernel, heads),
        out_shape=vmem(received.shape, BF16),
        in_specs=whole(3),
        out_specs=pl.BlockSpec(memory_space=pltpu.VMEM),
        compiler_params=pltpu.CompilerParams(vmem_limit_bytes=4 << 20),
        name="core_merge",
    )(*held(acc, stat, received))


def near_merge_kernel(heads, acc_ref, stat_ref, recv_ref, own_ref, own_stat_ref):
    dim = acc_ref.shape[2] // heads
    columns, m, l = merged(acc_ref[0], stat_ref[0, 0], stat_ref[0, 1], recv_ref[...], heads)
    for i, c in enumerate(columns):
        own_ref[:, pl.ds(i * dim, dim)] = c
    own_stat_ref[0] = m
    own_stat_ref[1] = l


def near_merge(acc, stat, received, heads):
    return pl.pallas_call(
        functools.partial(near_merge_kernel, heads),
        out_shape=(vmem(acc.shape[1:], F32), vmem(stat.shape[1:], F32)),
        in_specs=whole(3),
        out_specs=whole(2),
        cost_estimate=pl.CostEstimate(flops=1 << 22, bytes_accessed=0, transcendentals=0),
        compiler_params=pltpu.CompilerParams(vmem_limit_bytes=4 << 20),
        name="near_merge",
    )(*held(acc, stat, received))


def final_merge_kernel(heads, n, own_ref, stat_ref, *refs):
    recv, out_ref = refs[:n], refs[n]
    width = own_ref.shape[1]
    dim = width // heads
    stats = [(stat_ref[0], stat_ref[1])] + [unpack_stats(r[:, pl.ds(width, LANES)], heads) for r in recv]
    top = functools.reduce(jnp.maximum, [m for m, _ in stats])
    weights = [jnp.exp(m - top) for m, _ in stats]
    inverse = 1.0 / sum(w * l for w, (_, l) in zip(weights, stats))
    weights = [w * inverse for w in weights]
    for i in range(heads):
        columns = pl.ds(i * dim, dim)
        total = weights[0][:, i : i + 1] * own_ref[:, columns]
        for w, r in zip(weights[1:], recv):
            total = total + w[:, i : i + 1] * r[:, columns].astype(F32)
        out_ref[:, columns] = total.astype(BF16)


def final_merge(own, stat, received, heads):
    return pl.pallas_call(
        functools.partial(final_merge_kernel, heads, len(received)),
        out_shape=vmem(own.shape, BF16),
        in_specs=whole(2 + len(received)),
        out_specs=pl.BlockSpec(memory_space=pltpu.VMEM),
        compiler_params=pltpu.CompilerParams(vmem_limit_bytes=8 << 20),
        name="final_merge",
    )(*held(own, stat, *received))


def project_kernel(n, *refs):
    blocks, w_ref = refs[:n], refs[n]
    send_ref, keep_ref, lhs = refs[n + 1 :]
    tokens = blocks[0].shape[0]
    twist = lax.axis_index("dp") ^ lax.axis_index("tensor")
    for kd in range(n):
        at = twist ^ kd
        lhs[pl.ds(pl.multiple_of(at * tokens, tokens), tokens), :] = blocks[kd][...]
    out = jnp.dot(lhs[...], w_ref[...], preferred_element_type=F32)
    for kt in range(n):
        piece = out[kt * tokens : (kt + 1) * tokens]
        if kt % 2:
            send_ref[kt // 2] = piece.astype(BF16)
        else:
            keep_ref[kt // 2] = piece


def project(blocks, weight):
    n, (tokens, width), columns = len(blocks), blocks[0].shape, weight.shape[1]
    shape = (n // 2, tokens, columns)
    return pl.pallas_call(
        functools.partial(project_kernel, n),
        out_shape=(vmem(shape, BF16), vmem(shape, F32)),
        in_specs=whole(n + 1),
        out_specs=whole(2),
        scratch_shapes=[pltpu.VMEM((n * tokens, width), BF16)],
        cost_estimate=pl.CostEstimate(flops=2 * n * tokens * width * columns, bytes_accessed=0, transcendentals=0),
        compiler_params=pltpu.CompilerParams(vmem_limit_bytes=8 << 20),
        name="project",
    )(*held(*blocks, weight))


def swap(x, axes, n, k):
    return lax.ppermute(x, axes, [(i, i ^ k) for i in range(n)])


def on_device(queries, keys, values, cached_length, out_weight):
    _, _, model = queries.shape
    q_heads = model // keys.shape[3]
    tensor, groups, dps = lax.axis_size("tensor"), lax.axis_size("group"), lax.axis_size("dp")
    halves, heads = tensor // 2, q_heads // tensor

    plan = Attention(queries, keys, tensor)
    far = list(range(3, tensor, 2))
    order = far + [c - 1 for c in far] + [1, 0]
    send, *loaded = plan.first(far, order, cached_length, queries, keys, values)
    received = swap(send, "tensor", tensor, 1)
    acc, stat = plan.keep([c - 1 for c in far], *loaded)
    send = core_merge(acc, stat, received, heads)
    arrived = []
    for k in range(1, halves):
        arrived.append(swap(send[k - 1], "tensor", tensor, 2 * k))
    near = plan.send(1, *loaded)
    near = swap(near, "tensor", tensor, 1)
    acc, stat = plan.keep([0], *loaded)
    own, stat = near_merge(acc, stat, near, heads)
    attended = final_merge(own, stat, arrived, heads)

    weight = fetch(attended, out_weight)
    line = [attended]
    for k in range(1, dps):
        line.append(swap(attended, "dp", dps, k))
    plane, n = ("group", "tensor"), groups * tensor
    sums = []
    for kg in range(groups):
        blocks = line
        if kg:
            blocks = []
            for b in line:
                blocks.append(swap(b, "group", groups, kg))
        send, keep = project(blocks, weight)
        both = keep + swap(send, "tensor", tensor, 1).astype(F32)
        total = 0.0 if kg else both[0]
        for kx in range(halves):
            if kg or kx:
                total = total + swap(both[kx].astype(BF16), plane, n, kg * tensor + 2 * kx).astype(F32)
        sums.append(total)
    me = lax.axis_index("group")
    placed = []
    for g in range(groups):
        kept = sums[0]
        for kg in range(1, groups):
            kept = jnp.where(me ^ kg == g, sums[kg], kept)
        placed.append(kept)
    return jnp.stack(placed, axis=1).astype(BF16)


def solution(mesh):
    in_specs = (
        P(("group", "dp"), None, None),
        P(("group", "dp"), None, "tensor", None),
        P(("group", "dp"), None, "tensor", None),
        P(("group", "dp")),
        P("tensor", ("group", "dp")),
    )
    out_specs = P(("group", "tensor"), None, "dp")
    return jax.shard_map(
        on_device, mesh=mesh, in_specs=in_specs, out_specs=out_specs, check_vma=False
    )
```

```python
import functools
import math

import jax
import jax.numpy as jnp
from jax import lax
from jax.experimental import pallas as pl
from jax.experimental.pallas import tpu as pltpu
from jax.sharding import PartitionSpec as P


F32, BF16 = jnp.float32, jnp.bfloat16
LANES, SUBLANES = 128, 8
MASKED = -1e30
FETCH_FLOPS = 1 << 27


def vmem(shape, dtype):
    return pltpu.VMEM(shape, dtype)


def whole(n):
    return [pl.BlockSpec(memory_space=pltpu.VMEM)] * n


def held(*arrays):
    return [pltpu.with_memory_space_constraint(x, pltpu.VMEM) for x in arrays]


def in_hbm(*arrays):
    return [pltpu.with_memory_space_constraint(x, pltpu.HBM) for x in arrays]


def fetch_kernel(_, w_hbm, w_ref, sem):
    copy = pltpu.make_async_copy(w_hbm, w_ref, sem)
    copy.start()
    copy.wait()


def fetch(after, weight):
    return pl.pallas_call(
        fetch_kernel,
        out_shape=vmem(weight.shape, weight.dtype),
        in_specs=[pl.BlockSpec(memory_space=pltpu.VMEM), pl.BlockSpec(memory_space=pltpu.HBM)],
        out_specs=pl.BlockSpec(memory_space=pltpu.VMEM),
        scratch_shapes=[pltpu.SemaphoreType.DMA],
        cost_estimate=pl.CostEstimate(flops=FETCH_FLOPS, bytes_accessed=weight.size * 2, transcendentals=0),
        compiler_params=pltpu.CompilerParams(vmem_limit_bytes=1 << 20),
        name="fetch",
    )(*held(after), *in_hbm(weight))


def split3(x):
    hi = x.astype(BF16)
    rest = x - hi.astype(F32)
    mid = rest.astype(BF16)
    return hi, mid, (rest - mid.astype(F32)).astype(BF16)


def pack_stats(m, l, heads):
    lane = lax.broadcasted_iota(jnp.int32, m.shape, 1)
    out = jnp.zeros(m.shape, F32)
    for i, part in enumerate(split3(m) + split3(l)):
        term = jnp.where(lane < heads, part.astype(F32), 0.0)
        out = out + (pltpu.roll(term, i * heads, 1) if i else term)
    return out.astype(BF16)


def unpack_stats(packed, heads):
    x = packed.astype(F32)
    lane = lax.broadcasted_iota(jnp.int32, x.shape, 1)

    def term(i):
        return pltpu.roll(x, LANES - i * heads, 1) if i else x

    m = (term(0) + term(1)) + term(2)
    l = (term(3) + term(4)) + term(5)
    return jnp.where(lane < heads, m, 0.0), jnp.where(lane < heads, l, 0.0)


def attend(heads, join, q_ref, k_ref, v_ref, gap_ref, f_scr, o_ref, s_ref):
    rows, steps, _ = q_ref.shape
    span, _, dim = k_ref.shape[1:]
    parts, m_rows = heads // join, join * steps
    scale = 1.0 / math.sqrt(dim)
    lane = lax.broadcasted_iota(jnp.int32, (m_rows, LANES), 1)
    srow = lax.broadcasted_iota(jnp.int32, (m_rows, LANES), 0)
    allowed = [gap_ref[r] < 1 for r in range(rows)]
    units = [(part, r) for part in range(parts) for r in range(rows)]
    for u, (part, r) in enumerate(units):
        for j in range(join):
            f_scr[u, pl.ds(j * steps, steps), :] = q_ref[r, :, pl.ds((part * join + j) * dim, dim)].astype(F32)
    s = [
        lax.dot_general(
            f_scr[u].astype(BF16), k_ref[r, part * span // parts],
            (((1,), (1,)), ((), ())), preferred_element_type=F32,
        )
        for u, (part, r) in enumerate(units)
    ]
    s = [jnp.where(allowed[r], x * scale, MASKED) for x, (_, r) in zip(s, units)]
    m = [jnp.max(x, axis=1, keepdims=True) for x in s]
    p = [jnp.where(allowed[r], jnp.exp(x - y), 0.0) for x, y, (_, r) in zip(s, m, units)]
    l = [jnp.sum(x, axis=1, keepdims=True) for x in p]
    o = [
        jnp.dot(x.astype(BF16), v_ref[r, part * span // parts], preferred_element_type=F32)
        for x, (part, r) in zip(p, units)
    ]
    for x, (part, r) in zip(o, units):
        for j in range(join):
            o_ref[pl.ds(r * steps, steps), pl.ds((part * join + j) * dim, dim)] = x[j * steps : (j + 1) * steps]
    for i, stat in enumerate((m, l)):
        for r in range(rows):
            total = 0.0
            for x, (part, at) in zip(stat, units):
                if at == r:
                    x = jnp.where(lane == part * join + srow // steps, x, 0.0)
                    for b in range(0, m_rows, SUBLANES):
                        total = total + x[b : b + SUBLANES]
            shift = steps
            while shift < SUBLANES:
                total = total + pltpu.roll(total, shift, 0)
                shift *= 2
            s_ref[i, pl.ds(r * steps, steps), :] = total[:steps]


def attend_packed(heads, join, q_ref, k_ref, v_ref, gap_ref, f_scr, o_scr, s_scr, send_ref):
    attend(heads, join, q_ref, k_ref, v_ref, gap_ref, f_scr, o_scr, s_scr)
    width = o_scr.shape[1]
    send_ref[:, pl.ds(0, width)] = o_scr[...].astype(BF16)
    send_ref[:, pl.ds(width, LANES)] = pack_stats(s_scr[0], s_scr[1], heads)


def first_kernel(heads, join, chunks, order, len_hbm, q_hbm, k_hbm, v_hbm, send_ref, q_ref, k_ref, v_ref, gap_ref, len_scr, f_scr, o_scr, s_scr, sems):
    rows = q_hbm.shape[0]
    kv_heads, cache, dim = k_hbm.shape[1:]
    q_heads = q_hbm.shape[2] // dim
    tensor, width, span = q_heads // heads, heads * dim, k_ref.shape[2]
    me = lax.axis_index("tensor")
    copies = []
    for chunk in range(tensor):
        owner = me ^ chunk
        kv = owner * heads // (q_heads // kv_heads)
        copies.append([
            pltpu.make_async_copy(q_hbm.at[:, :, pl.ds(pl.multiple_of(owner * width, width), width)], q_ref.at[chunk], sems.at[0, chunk]),
            pltpu.make_async_copy(k_hbm.at[:, pl.ds(kv, span)], k_ref.at[chunk], sems.at[1, chunk]),
            pltpu.make_async_copy(v_hbm.at[:, pl.ds(kv, span)], v_ref.at[chunk], sems.at[2, chunk]),
        ])
    limits = pltpu.make_async_copy(len_hbm, len_scr, sems.at[3, 0])
    limits.start()
    for chunk in order:
        for copy in copies[chunk]:
            copy.start()
    limits.wait()
    shape = gap_ref.shape[1:]
    row = lax.broadcasted_iota(jnp.int32, shape, 0)
    steps = q_hbm.shape[1]
    position = me * cache + lax.broadcasted_iota(jnp.int32, shape, 1) - row % steps
    for r in range(rows):
        gap_ref[r] = position - len_scr[r]
    for i, chunk in enumerate(chunks):
        for copy in copies[chunk]:
            copy.wait()
        attend_packed(heads, join, q_ref.at[chunk], k_ref.at[chunk], v_ref.at[chunk], gap_ref, f_scr.at[i], o_scr.at[i], s_scr.at[i], send_ref.at[i])
    for chunk in order:
        if chunk not in chunks:
            for copy in copies[chunk]:
                copy.wait()


def send_kernel(heads, join, chunk, q_ref, k_ref, v_ref, gap_ref, send_ref, f_scr, o_scr, s_scr):
    attend_packed(heads, join, q_ref.at[chunk], k_ref.at[chunk], v_ref.at[chunk], gap_ref, f_scr, o_scr, s_scr, send_ref)


def keep_kernel(heads, join, chunks, q_ref, k_ref, v_ref, gap_ref, acc_ref, stat_ref, f_scr):
    for i, c in enumerate(chunks):
        attend(heads, join, q_ref.at[c], k_ref.at[c], v_ref.at[c], gap_ref, f_scr.at[i], acc_ref.at[i], stat_ref.at[i])


class Attention:
    def __init__(self, queries, keys, tensor):
        self.rows, self.steps, model = queries.shape
        kv_heads, self.cache, self.dim = keys.shape[1:]
        q_heads = model // self.dim
        per_kv = q_heads // kv_heads
        self.tensor, self.heads = tensor, q_heads // tensor
        self.join, self.span = min(self.heads, per_kv), max(1, self.heads // per_kv)
        self.width, self.tokens = self.heads * self.dim, self.rows * self.steps
        self.m_rows = self.join * self.steps

    def scratch(self, n):
        lead = (n,) if n else ()
        return [
            pltpu.VMEM((*lead, self.rows * self.heads // self.join, self.m_rows, self.dim), F32),
            pltpu.VMEM((*lead, self.tokens, self.width), F32),
            pltpu.VMEM((*lead, 2, self.tokens, LANES), F32),
        ]

    def options(self, n):
        work = 4 * n * self.tokens * self.width * self.cache
        return dict(
            cost_estimate=pl.CostEstimate(flops=4 * work, bytes_accessed=0, transcendentals=0),
            compiler_params=pltpu.CompilerParams(vmem_limit_bytes=8 << 20),
        )

    def first(self, chunks, order, lengths, queries, keys, values):
        cached = (self.tensor, self.rows, self.span, self.cache, self.dim)
        return pl.pallas_call(
            functools.partial(first_kernel, self.heads, self.join, chunks, order),
            out_shape=(
                vmem((len(chunks), self.tokens, self.width + LANES), BF16),
                vmem((self.tensor, self.rows, self.steps, self.width), BF16),
                vmem(cached, BF16),
                vmem(cached, BF16),
                vmem((self.rows, self.m_rows, self.cache), jnp.int32),
            ),
            in_specs=[pl.BlockSpec(memory_space=pltpu.HBM)] * 4,
            out_specs=whole(5),
            scratch_shapes=[pltpu.SMEM((self.rows,), jnp.int32)] + self.scratch(len(chunks)) + [pltpu.SemaphoreType.DMA((4, self.tensor))],
            name="attend_first",
            **self.options(len(chunks)),
        )(*in_hbm(lengths, queries, keys, values))

    def send(self, chunk, *loaded):
        return pl.pallas_call(
            functools.partial(send_kernel, self.heads, self.join, chunk),
            out_shape=vmem((self.tokens, self.width + LANES), BF16),
            in_specs=whole(4),
            out_specs=pl.BlockSpec(memory_space=pltpu.VMEM),
            scratch_shapes=self.scratch(0),
            name="attend_send",
            **self.options(1),
        )(*held(*loaded))

    def keep(self, chunks, *loaded):
        n = len(chunks)
        return pl.pallas_call(
            functools.partial(keep_kernel, self.heads, self.join, chunks),
            out_shape=(vmem((n, self.tokens, self.width), F32), vmem((n, 2, self.tokens, LANES), F32)),
            in_specs=whole(4),
            out_specs=whole(2),
            scratch_shapes=self.scratch(n)[:1],
            name="attend_keep",
            **self.options(n),
        )(*held(*loaded))


def merged(acc, m, l, received, heads):
    width = acc.shape[1]
    dim = width // heads
    m2, l2 = unpack_stats(received[:, width:], heads)
    top = jnp.maximum(m, m2)
    e1, e2 = jnp.exp(m - top), jnp.exp(m2 - top)
    columns = [
        e1[:, i : i + 1] * acc[:, i * dim : (i + 1) * dim]
        + e2[:, i : i + 1] * received[:, i * dim : (i + 1) * dim].astype(F32)
        for i in range(heads)
    ]
    return columns, top, e1 * l + e2 * l2


def core_merge_kernel(heads, acc_ref, stat_ref, recv_ref, send_ref):
    width = acc_ref.shape[2]
    dim = width // heads
    for k in range(acc_ref.shape[0]):
        columns, m, l = merged(acc_ref[k], stat_ref[k, 0], stat_ref[k, 1], recv_ref[k], heads)
        for i, c in enumerate(columns):
            send_ref[k, :, pl.ds(i * dim, dim)] = c.astype(BF16)
        send_ref[k, :, pl.ds(width, LANES)] = pack_stats(m, l, heads)


def core_merge(acc, stat, received, heads):
    return pl.pallas_call(
        functools.partial(core_merge_kernel, heads),
        out_shape=vmem(received.shape, BF16),
        in_specs=whole(3),
        out_specs=pl.BlockSpec(memory_space=pltpu.VMEM),
        compiler_params=pltpu.CompilerParams(vmem_limit_bytes=4 << 20),
        name="core_merge",
    )(*held(acc, stat, received))


def near_merge_kernel(heads, acc_ref, stat_ref, recv_ref, own_ref, own_stat_ref):
    dim = acc_ref.shape[2] // heads
    columns, m, l = merged(acc_ref[0], stat_ref[0, 0], stat_ref[0, 1], recv_ref[...], heads)
    for i, c in enumerate(columns):
        own_ref[:, pl.ds(i * dim, dim)] = c
    own_stat_ref[0] = m
    own_stat_ref[1] = l


def near_merge(acc, stat, received, heads):
    return pl.pallas_call(
        functools.partial(near_merge_kernel, heads),
        out_shape=(vmem(acc.shape[1:], F32), vmem(stat.shape[1:], F32)),
        in_specs=whole(3),
        out_specs=whole(2),
        cost_estimate=pl.CostEstimate(flops=1 << 22, bytes_accessed=0, transcendentals=0),
        compiler_params=pltpu.CompilerParams(vmem_limit_bytes=4 << 20),
        name="near_merge",
    )(*held(acc, stat, received))


def final_merge_kernel(heads, n, own_ref, stat_ref, *refs):
    recv, out_ref = refs[:n], refs[n]
    width = own_ref.shape[1]
    dim = width // heads
    stats = [(stat_ref[0], stat_ref[1])] + [unpack_stats(r[:, pl.ds(width, LANES)], heads) for r in recv]
    top = functools.reduce(jnp.maximum, [m for m, _ in stats])
    weights = [jnp.exp(m - top) for m, _ in stats]
    inverse = 1.0 / sum(w * l for w, (_, l) in zip(weights, stats))
    weights = [w * inverse for w in weights]
    for i in range(heads):
        columns = pl.ds(i * dim, dim)
        total = weights[0][:, i : i + 1] * own_ref[:, columns]
        for w, r in zip(weights[1:], recv):
            total = total + w[:, i : i + 1] * r[:, columns].astype(F32)
        out_ref[:, columns] = total.astype(BF16)


def final_merge(own, stat, received, heads):
    return pl.pallas_call(
        functools.partial(final_merge_kernel, heads, len(received)),
        out_shape=vmem(own.shape, BF16),
        in_specs=whole(2 + len(received)),
        out_specs=pl.BlockSpec(memory_space=pltpu.VMEM),
        compiler_params=pltpu.CompilerParams(vmem_limit_bytes=8 << 20),
        name="final_merge",
    )(*held(own, stat, *received))


def project_kernel(n, *refs):
    blocks, w_ref = refs[:n], refs[n]
    send_ref, keep_ref, lhs = refs[n + 1 :]
    tokens = blocks[0].shape[0]
    twist = lax.axis_index("dp") ^ lax.axis_index("tensor")
    for kd in range(n):
        at = twist ^ kd
        lhs[pl.ds(pl.multiple_of(at * tokens, tokens), tokens), :] = blocks[kd][...]
    out = jnp.dot(lhs[...], w_ref[...], preferred_element_type=F32)
    for kt in range(n):
        piece = out[kt * tokens : (kt + 1) * tokens]
        if kt % 2:
            send_ref[kt // 2] = piece.astype(BF16)
        else:
            keep_ref[kt // 2] = piece


def project(blocks, weight):
    n, (tokens, width), columns = len(blocks), blocks[0].shape, weight.shape[1]
    shape = (n // 2, tokens, columns)
    return pl.pallas_call(
        functools.partial(project_kernel, n),
        out_shape=(vmem(shape, BF16), vmem(shape, F32)),
        in_specs=whole(n + 1),
        out_specs=whole(2),
        scratch_shapes=[pltpu.VMEM((n * tokens, width), BF16)],
        cost_estimate=pl.CostEstimate(flops=2 * n * tokens * width * columns, bytes_accessed=0, transcendentals=0),
        compiler_params=pltpu.CompilerParams(vmem_limit_bytes=8 << 20),
        name="project",
    )(*held(*blocks, weight))


def swap(x, axes, n, k):
    return lax.ppermute(x, axes, [(i, i ^ k) for i in range(n)])


def on_device(queries, keys, values, cached_length, out_weight):
    _, _, model = queries.shape
    q_heads = model // keys.shape[3]
    tensor, groups, dps = lax.axis_size("tensor"), lax.axis_size("group"), lax.axis_size("dp")
    halves, heads = tensor // 2, q_heads // tensor

    plan = Attention(queries, keys, tensor)
    far = list(range(3, tensor, 2))
    order = far + [c - 1 for c in far] + [1, 0]
    send, *loaded = plan.first(far, order, cached_length, queries, keys, values)
    received = swap(send, "tensor", tensor, 1)
    acc, stat = plan.keep([c - 1 for c in far], *loaded)
    send = core_merge(acc, stat, received, heads)
    arrived = []
    for k in range(1, halves):
        arrived.append(swap(send[k - 1], "tensor", tensor, 2 * k))
    near = plan.send(1, *loaded)
    near = swap(near, "tensor", tensor, 1)
    acc, stat = plan.keep([0], *loaded)
    own, stat = near_merge(acc, stat, near, heads)
    attended = final_merge(own, stat, arrived, heads)

    weight = fetch(attended, out_weight)
    plane, n = ("group", "tensor"), groups * tensor
    crossed = [attended]
    for kg in range(1, groups):
        crossed.append(swap(attended, "group", groups, kg))
    columns = [[b] + [None] * (dps - 1) for b in crossed]
    for k in range(1, dps):
        if k == 1:
            got = swap(jnp.stack(crossed), "dp", dps, k)
            for kg in range(groups):
                columns[kg][k] = got[kg]
            continue
        columns[0][k] = swap(attended, "dp", dps, k)
        for kg in range(1, groups):
            columns[kg][k] = swap(columns[0][k], "group", groups, kg)
    sums = []
    for kg, blocks in enumerate(columns):
        send, keep = project(blocks, weight)
        both = keep + swap(send, "tensor", tensor, 1).astype(F32)
        total = 0.0 if kg else both[0]
        for kx in range(halves):
            if kg or kx:
                total = total + swap(both[kx].astype(BF16), plane, n, kg * tensor + 2 * kx).astype(F32)
        sums.append(total)
    me = lax.axis_index("group")
    placed = []
    for g in range(groups):
        kept = sums[0]
        for kg in range(1, groups):
            kept = jnp.where(me ^ kg == g, sums[kg], kept)
        placed.append(kept)
    return jnp.stack(placed, axis=1).astype(BF16)


def solution(mesh):
    in_specs = (
        P(("group", "dp"), None, None),
        P(("group", "dp"), None, "tensor", None),
        P(("group", "dp"), None, "tensor", None),
        P(("group", "dp")),
        P("tensor", ("group", "dp")),
    )
    out_specs = P(("group", "tensor"), None, "dp")
    return jax.shard_map(
        on_device, mesh=mesh, in_specs=in_specs, out_specs=out_specs, check_vma=False
    )
```
